32 devices in a mesh: lat: 16 (over z, y, x), lon: 2 (over core).
Axes of the slice: x: 2, y: 2, z: 4, core: 2. Of those that a mesh axis runs over, the one named last changes fastest.
Arguments:
- fields: bfloat16 [2048, 2, 1024], P('lat', 'lon'), may hold values from -6 to 6
- proj_x: bfloat16 [1024, 1024], P('lon'), may hold values from -0.1875 to 0.1875
- proj_z: bfloat16 [1024, 1024], P('lon'), may hold values from -0.1875 to 0.1875
- proj_bc: bfloat16 [1024, 128], P('lon'), may hold values from -0.1875 to 0.1875
- proj_dt: bfloat16 [1024, 16], P('lon'), may hold values from -1 to 1
- conv_x: float32 [4, 1024], replicated, may hold values from -3 to 3
- conv_bc: float32 [4, 128], replicated, may hold values from -3 to 3
- dt_bias: float32 [16], replicated, may hold values from -1 to 0.5
- log_rate: float32 [16], replicated, may hold values from -12 to -2.7
- norm_gain: float32 [1024], replicated, may hold values from 0.1 to 1.9
- proj_out: bfloat16 [1024, 1024], P('lon'), may hold values from -0.1875 to 0.1875
Outputs:
- mixer_out: bfloat16 [2048, 2, 1024], P('lat', 'lon')
The draws below stay inside these ranges and needn't reach their ends.
All inputs are finite; a program needn't handle non-finite values.
Results may differ from the reference program's by a relative error of at most 0.012.
Values may be sent and summed in bfloat16 or wider, within the bound.
A program may use at most 64 MiB of HBM per device.

```python
import jax
import jax.numpy as jnp
from jax import lax

D = 1024
HEADS = 16
HEAD_DIM = 64
STATE = 64
KERNEL = 4
LAT_DEV = 128
INNER = 1024
LAT = 2048
LON = 2


def shared_direction(key):
    base_key = jax.random.fold_in(key, 101)
    key_dir, key_size, key_sign = jax.random.split(base_key, 3)
    direction = jax.random.normal(key_dir, (D,), jnp.float32)
    direction = direction / jnp.sqrt(jnp.sum(direction * direction))
    head_size = jax.random.uniform(key_size, (HEADS,), jnp.float32, 0.4, 0.7)
    head_sign = jnp.where(jax.random.uniform(key_sign, (HEADS,), jnp.float32) < 0.5, -1.0, 1.0)
    return (direction, head_size * head_sign)


def draw_fields(key, part):
    direction, head_weight = shared_direction(key)
    own_key = jax.random.fold_in(key, 202)
    key_noise, key_level, key_jitter = jax.random.split(own_key, 3)
    segment = max(1, 3 * LAT_DEV // 2)
    level_count = LAT // segment + 1
    noise = jax.random.normal(key_noise, (LAT, LON, D), jnp.float32)
    levels = jax.random.uniform(key_level, (level_count,), jnp.float32, -3.5, 3.5)
    row_level = levels[jnp.arange(LAT) // segment]
    along = row_level + 0.5 * jax.random.normal(key_jitter, (LAT,), jnp.float32)
    values = noise + along[:, None, None] * direction[None, None, :]
    return jnp.clip(values, -6.0, 6.0).astype(jnp.bfloat16)


def draw_proj_dt(key, part):
    direction, head_weight = shared_direction(key)
    own_key = jax.random.fold_in(key, 303)
    base = jax.random.normal(own_key, (D, HEADS), jnp.float32) / jnp.sqrt(16.0 * D)
    values = base + direction[:, None] * head_weight[None, :]
    return jnp.clip(values, -1.0, 1.0).astype(jnp.bfloat16)


def draw_log_rate(key, part):
    key_slow, key_pick, key_long, key_short = jax.random.split(jax.random.fold_in(key, 17), 4)
    slow_share = 0.5
    slow_heads = jax.random.uniform(key_slow, (HEADS,), jnp.float32) < slow_share
    picked = jnp.arange(HEADS) == jax.random.randint(key_pick, (), 0, HEADS)
    slow_heads = jnp.logical_or(slow_heads, picked)
    long_reach = jnp.exp(jax.random.uniform(key_long, (HEADS,), jnp.float32, jnp.log(0.2), jnp.log(1.0)))
    short_reach = jnp.exp(jax.random.uniform(key_short, (HEADS,), jnp.float32, jnp.log(25.0), jnp.log(50.0)))
    rates = jnp.where(slow_heads, long_reach / (0.6 * LAT), 1.0 / (0.6 * short_reach))
    return jnp.log(rates).astype(jnp.float32)


def block_levels(stream_key, shape, cuts, least, high):
    gain = 1.0
    for dim, shards_of in cuts:
        heights = jax.random.uniform(jax.random.fold_in(jax.random.fold_in(stream_key, 6), dim), (shards_of,), jnp.float32, least / len(cuts), high / len(cuts))
        gain = gain * jnp.repeat(jnp.exp(heights), shape[dim] // shards_of).reshape((-1,) + (1,) * (len(shape) - 1 - dim))
    return gain


def normal_values(stream_key, shape, scale, limit, cuts=(), kind=jnp.bfloat16):
    values = jax.random.normal(stream_key, shape, jnp.float32) * scale
    if len(cuts) > 0:
        values = block_levels(stream_key, shape, cuts, -0.22, 0.18) * values
    return jnp.clip(values, min=-limit, max=limit).astype(kind)


def setup_inputs(seed: int = 0) -> dict:
    seeds = jax.random.split(jax.random.key(seed), 12)
    fields = draw_fields(jax.random.fold_in(seeds[11], 71), 0)
    proj_x = normal_values(seeds[1], (D, INNER), D ** -0.5, 0.1875, ((0, 2),))
    proj_z = normal_values(seeds[2], (D, INNER), D ** -0.5, 0.1875, ((0, 2),))
    proj_bc = normal_values(seeds[3], (D, 2 * STATE), D ** -0.5, 0.1875, ((0, 2),))
    proj_dt = draw_proj_dt(jax.random.fold_in(seeds[11], 71), 0)
    conv_x = normal_values(seeds[5], (KERNEL, INNER), KERNEL ** -0.5, 3.0, (), jnp.float32)
    conv_bc = normal_values(seeds[6], (KERNEL, 2 * STATE), KERNEL ** -0.5, 3.0, (), jnp.float32)
    dt_bias = jnp.clip(jax.random.uniform(seeds[7], (HEADS,), jnp.float32, -1.0, 0.5), -1.0, 0.5)
    log_rate = draw_log_rate(jax.random.fold_in(seeds[11], 71), 0)
    norm_gain = jnp.clip(1.0 + 0.18 * jax.random.normal(seeds[9], (INNER,), jnp.float32), 0.1, 1.9)
    proj_out = normal_values(seeds[10], (INNER, D), INNER ** -0.5, 0.1875, ((0, 2),))
    return {"fields": fields, "proj_x": proj_x, "proj_z": proj_z, "proj_bc": proj_bc, "proj_dt": proj_dt, "conv_x": conv_x, "conv_bc": conv_bc, "dt_bias": dt_bias, "log_rate": log_rate, "norm_gain": norm_gain, "proj_out": proj_out}


norm_epsilon = 1e-05
highest = lax.Precision.HIGHEST

def causal_conv(values, kernel):
    out_rows = values.shape[0] - kernel.shape[0] + 1
    acc_sum = jnp.zeros((out_rows,) + values.shape[1:], jnp.float32)
    for offset in range(kernel.shape[0]):
        acc_sum = acc_sum + kernel[offset] * values[offset:offset + out_rows]
    return jax.nn.silu(acc_sum).astype(jnp.bfloat16)

def band_mix(head_inner, input_b, read_c, step_dt, log_step, state_in):
    length = head_inner.shape[0]
    cumulative = jnp.cumsum(log_step, axis=0)
    causal = jnp.arange(length)[:, None] >= jnp.arange(length)[None, :]
    decay_gap = cumulative[:, None] - cumulative[None, :]
    decay = jnp.exp(jnp.where(causal[:, :, None, None], decay_gap, -jnp.inf))
    scores = jnp.einsum('tcn,scn->tsc', read_c, input_b, precision=highest)
    weights = decay * scores[:, :, :, None] * step_dt[None]
    diag_out = jnp.einsum('tsch,schp->tchp', weights, head_inner, precision=highest)
    state_out = jnp.einsum('tcn,chnp->tchp', read_c, state_in, precision=highest) * jnp.exp(cumulative)[..., None]
    end_weight = jnp.exp(cumulative[-1][None] - cumulative) * step_dt
    end_state = jnp.einsum('sch,scn,schp->chnp', end_weight, input_b, head_inner, precision=highest)
    return (diag_out + state_out, end_state, cumulative[-1])

def reference(fields, proj_x, proj_z, proj_bc, proj_dt, conv_x, conv_bc, dt_bias, log_rate, norm_gain, proj_out):
    lat_count, lon_count, model_width = fields.shape
    flat_rows = fields.reshape(lat_count * lon_count, model_width)

    def project(weight):
        return jnp.dot(flat_rows, weight, preferred_element_type=jnp.float32).astype(jnp.bfloat16).reshape(lat_count, lon_count, -1)
    inner_pre = project(proj_x)
    gate_pre = project(proj_z)
    bc_pre = project(proj_bc)
    dt_pre = project(proj_dt)
    margin = KERNEL - 1

    def extend(values):
        return jnp.concatenate([jnp.zeros((margin,) + values.shape[1:], jnp.float32), values.astype(jnp.float32)], 0)
    inner_act = causal_conv(extend(inner_pre), conv_x)
    bc_act = causal_conv(extend(bc_pre), conv_bc)
    step_dt = jax.nn.softplus(dt_pre.astype(jnp.float32) + dt_bias)
    log_step = -jnp.exp(log_rate) * step_dt
    head_count = log_rate.shape[0]
    blocks = lat_count // LAT_DEV

    def block_view(values):
        return values.reshape((blocks, LAT_DEV) + values.shape[1:])
    head_inner = inner_act.astype(jnp.float32).reshape(lat_count, lon_count, head_count, HEAD_DIM)
    inputs = (block_view(head_inner), block_view(bc_act[..., :STATE].astype(jnp.float32)), block_view(bc_act[..., STATE:].astype(jnp.float32)), block_view(step_dt), block_view(log_step))

    def advance(carried, pieces):
        band_out, end_state, band_total = band_mix(pieces[0], pieces[1], pieces[2], pieces[3], pieces[4], carried)
        return (jnp.exp(band_total)[..., None, None] * carried + end_state, band_out)
    start_state = jnp.zeros((lon_count, head_count, STATE, HEAD_DIM), jnp.float32)
    final_state, band_outs = lax.scan(advance, start_state, inputs)
    mixed_heads = band_outs.reshape(lat_count, lon_count, head_count * HEAD_DIM)
    gated_out = mixed_heads * jax.nn.silu(gate_pre.astype(jnp.float32))
    normed = gated_out * lax.rsqrt(lax.optimization_barrier(jnp.mean(gated_out * gated_out, -1, keepdims=True)) + norm_epsilon) * norm_gain
    hidden = normed.astype(jnp.bfloat16).reshape(lat_count * lon_count, -1)
    result = jnp.dot(hidden, proj_out, preferred_element_type=jnp.float32).astype(jnp.bfloat16)
    return result.reshape(lat_count, lon_count, model_width)
```

```python
import functools

import jax
import jax.numpy as jnp
from jax import lax
from jax.experimental import pallas as pl
from jax.experimental.pallas import tpu as pltpu
from jax.sharding import PartitionSpec as P

norm_epsilon = 1e-05
LANES = 128
HALO = 16
f32 = jnp.float32
bf16 = jnp.bfloat16
highest = lax.Precision.HIGHEST


def silu(v):
    return v / (1.0 + jnp.exp(-v))


def expand(values, spread):
    high = values.astype(bf16)
    low = (values - high.astype(f32)).astype(bf16)
    return jnp.dot(high, spread, preferred_element_type=f32) + jnp.dot(
        low, spread, preferred_element_type=f32
    )


def kernel(
    n_lat,
    n_lon,
    heads,
    fields,
    wx,
    wz,
    wbc,
    wdt,
    wo,
    cx,
    cbc,
    dtb,
    lrate,
    gain,
    out,
    fbuf,
    bx,
    bz,
    bbc,
    bdt,
    bo,
    accx,
    accz,
    accbc,
    accdt,
    prm,
    act,
    diag,
    dec,
    tbuf,
    trecv,
    sbuf,
    srecv,
    pbuf,
    precv,
    local_sem,
    lon_send,
    lon_recv,
    halo_send,
    halo_recv,
    t_send,
    t_recv,
    s_send,
    s_recv,
    p_send,
    p_recv,
):
    rows, width = fields.shape
    inner = wx.shape[1]
    state = wbc.shape[1] // 2
    taps = cx.shape[0]
    kr = wx.shape[0]
    head_dim = inner // heads
    blocks = inner // LANES
    per_block = LANES // head_dim
    split = n_lat // blocks
    piece = state // split
    me = lax.axis_index("lat")
    col = lax.axis_index("lon")

    barrier = pltpu.get_barrier_semaphore()
    for k in range(1, n_lon):
        pl.semaphore_signal(barrier, inc=1, device_id={"lon": lax.rem(col + k, n_lon)})

    def greet(k, carry):
        pl.semaphore_signal(barrier, inc=1, device_id={"lat": lax.rem(me + k, n_lat)})
        return carry

    lax.fori_loop(1, n_lat, greet, 0)

    weights = ((wbc, bbc), (wdt, bdt), (wx, bx), (wz, bz), (wo, bo))
    own = [pltpu.make_async_copy(fields, fbuf.at[pl.ds(HALO, rows)], local_sem.at[5])]
    for i, (src, dst) in enumerate(weights):
        own.append(pltpu.make_async_copy(src, dst.at[col], local_sem.at[i]))
    for c in own:
        c.start()
    pl.semaphore_wait(barrier, n_lat - 1 + n_lon - 1)

    halo = pltpu.make_async_remote_copy(
        src_ref=fields.at[pl.ds(rows - HALO, HALO)],
        dst_ref=fbuf.at[pl.ds(0, HALO)],
        send_sem=halo_send,
        recv_sem=halo_recv,
        device_id={"lat": lax.rem(me + 1, n_lat)},
    )
    halo.start()

    def lon_copy(i, k):
        src, dst = weights[i]
        return pltpu.make_async_remote_copy(
            src_ref=src,
            dst_ref=dst.at[col],
            send_sem=lon_send.at[i, k],
            recv_sem=lon_recv.at[i, k],
            device_id={"lon": lax.rem(col + k, n_lon)},
        )

    for i in range(5):
        for k in range(1, n_lon):
            lon_copy(i, k).start()

    def part(k):
        source = lax.rem(col + n_lon - k, n_lon)
        return source, pl.ds(pl.multiple_of(source * kr, LANES), kr)

    def arrived(i, k):
        if k > 0:
            lon_copy(i, k).wait_recv()

    for c in own:
        c.wait()
    halo.wait_recv()
    keep = jnp.where(me > 0, 1.0, 0.0).astype(bf16)
    fbuf[0:HALO, :] = fbuf[0:HALO, :] * keep

    def accumulate(k, buf, acc, first_row, step):
        source, columns = part(k)
        lhs = fbuf[first_row:, columns]
        total = buf.shape[2]
        for start in range(0, total, step):
            size = min(step, total - start)
            term = jnp.dot(lhs, buf[source, :, start : start + size], preferred_element_type=f32)
            if k > 0:
                term = term + acc[:, start : start + size]
            if k == n_lon - 1:
                term = term.astype(bf16).astype(f32)
            acc[:, start : start + size] = term

    accumulate(0, bbc, accbc, 0, 256)
    accumulate(0, bdt, accdt, HALO, 256)
    accumulate(0, bx, accx, 0, 256)

    for k in range(1, n_lon):
        arrived(0, k)
        accumulate(k, bbc, accbc, 0, 256)
    for k in range(1, n_lon):
        arrived(1, k)
        accumulate(k, bdt, accdt, HALO, 256)

    def conv(acc, kernel_ref, start, size):
        total = None
        for k in range(taps):
            first = HALO - taps + 1 + k
            term = kernel_ref[k : k + 1, start : start + size] * acc[
                first : first + rows, start : start + size
            ]
            total = term if total is None else total + term
        return silu(total)

    bc_act = conv(accbc, cbc, 0, 2 * state)
    lane = lax.broadcasted_iota(jnp.int32, (rows, 2 * state), 1)
    bc16 = bc_act.astype(bf16)
    bc_f = bc16.astype(f32)
    read = pltpu.roll(bc_f, state, 1).astype(bf16)
    b_only = jnp.where(lane < state, bc_f, 0.0).astype(bf16)
    bc_t = bc_f.T.astype(bf16)

    prm[...] = jnp.zeros_like(prm)
    prm[0:1, 0:heads] = dtb[...]
    prm[1:2, 0:heads] = lrate[...]
    dec[0] = jnp.zeros((rows, LANES), f32)
    dec[0, :, 0:heads] = accdt[...]
    pre = dec[0] + prm[0:1, :]
    step_dt = jnp.maximum(pre, 0.0) + jnp.log1p(jnp.exp(-jnp.abs(pre)))
    log_step = -jnp.exp(prm[1:2, :]) * step_dt
    t_idx = lax.broadcasted_iota(jnp.int32, (rows, rows), 0)
    s_idx = lax.broadcasted_iota(jnp.int32, (rows, rows), 1)
    causal = t_idx >= s_idx
    cum = jnp.dot(
        jnp.where(causal, 1.0, 0.0), log_step, precision=highest, preferred_element_type=f32
    )
    dec[0] = cum
    dec[1] = cum.T
    dec[2] = step_dt.T
    band_total = cum[rows - 1 : rows, :]
    spread = jnp.where(
        lax.broadcasted_iota(jnp.int32, (LANES, inner), 1) // head_dim
        == lax.broadcasted_iota(jnp.int32, (LANES, inner), 0),
        1.0,
        0.0,
    ).astype(bf16)
    band_decay = expand(jnp.broadcast_to(jnp.exp(band_total), (8, LANES)), spread)
    for j in range(n_lat):
        c = j % blocks
        tbuf[j] = band_decay[:, c * LANES : (c + 1) * LANES]
    trecv[me] = tbuf[me]

    def exchange(k, buf, dst, send, recv):
        to = lax.rem(me + k, n_lat)
        return pltpu.make_async_remote_copy(
            src_ref=buf.at[to],
            dst_ref=dst.at[me],
            send_sem=send.at[to],
            recv_sem=recv.at[me],
            device_id={"lat": to},
        )

    def incoming(source, buf, dst, send, recv):
        return pltpu.make_async_remote_copy(
            src_ref=buf.at[source],
            dst_ref=dst.at[source],
            send_sem=send.at[source],
            recv_sem=recv.at[source],
            device_id={"lat": source},
        )

    def send_t(k, carry):
        exchange(k, tbuf, trecv, t_send, t_recv).start()
        return carry

    lax.fori_loop(1, n_lat, send_t, 0)

    scores = lax.dot_general(
        read, b_only, (((1,), (1,)), ((), ())), preferred_element_type=f32
    )
    end_weight = expand(jnp.exp(band_total - cum) * step_dt, spread)

    for k in range(1, n_lon):
        arrived(2, k)
        accumulate(k, bx, accx, 0, 256)
    for c in range(blocks):
        lanes = slice(c * LANES, (c + 1) * LANES)
        block = conv(accx, cx, c * LANES, LANES).astype(bf16)
        act[:, lanes] = block
        weighted = (block.astype(f32) * end_weight[:, lanes]).astype(bf16)
        end_state = jnp.dot(bc_t, weighted, preferred_element_type=f32)
        for r in range(split):
            sbuf[r * blocks + c] = end_state[r * piece : (r + 1) * piece, :].astype(bf16)
    srecv[me] = sbuf[me]

    def send_s(k, carry):
        exchange(k, sbuf, srecv, s_send, s_recv).start()
        return carry

    lax.fori_loop(1, n_lat, send_s, 0)

    half = lax.broadcasted_iota(jnp.int32, (rows, LANES), 1) // head_dim
    for c in range(blocks):
        lanes = slice(c * LANES, (c + 1) * LANES)
        mixed = None
        for g in range(per_block):
            h = c * per_block + g
            gap = dec[0, :, h : h + 1] - dec[1, h : h + 1, :]
            decay = jnp.exp(jnp.where(causal, gap, -jnp.inf))
            mix = (decay * scores * dec[2, h : h + 1, :]).astype(bf16)
            term = jnp.dot(mix, act[:, lanes], preferred_element_type=f32)
            mixed = term if mixed is None else jnp.where(half == g, term, mixed)
        diag[:, lanes] = mixed
    start_decay = jnp.exp(cum)

    carried = jnp.zeros((piece, LANES), f32)
    for d in range(n_lat):

        @pl.when(me != d)
        def _():
            incoming(d, tbuf, trecv, t_send, t_recv).wait_recv()
            incoming(d, sbuf, srecv, s_send, s_recv).wait_recv()

        pbuf[d] = carried.astype(bf16)
        carried = trecv[d][0:1, :] * carried + srecv[d].astype(f32)
    precv[me] = pbuf[me]

    def send_p(k, carry):
        exchange(k, pbuf, precv, p_send, p_recv).start()
        return carry

    lax.fori_loop(1, n_lat, send_p, 0)

    accumulate(0, bz, accz, HALO, 256)
    for k in range(1, n_lon):
        arrived(3, k)
        accumulate(k, bz, accz, HALO, 256)
    for c in range(blocks):
        lanes = slice(c * LANES, (c + 1) * LANES)
        accz[:, lanes] = silu(accz[:, lanes])
        accx[0:rows, lanes] = expand(start_decay, spread[:, lanes])
    for k in range(1, n_lon):
        arrived(4, k)

    def take_p(k, carry):
        incoming(lax.rem(me + k, n_lat), pbuf, precv, p_send, p_recv).wait_recv()
        return carry

    lax.fori_loop(1, n_lat, take_p, 0)

    square = jnp.zeros((rows, LANES), f32)
    for c in range(blocks):
        lanes = slice(c * LANES, (c + 1) * LANES)
        prefix = jnp.concatenate([precv[r * blocks + c] for r in range(split)], axis=0)
        lower = jnp.concatenate([jnp.zeros_like(prefix), prefix], axis=0)
        y = jnp.dot(bc16, lower, preferred_element_type=f32) * accx[0:rows, lanes] + diag[:, lanes]
        gated = y * accz[:, lanes]
        diag[:, lanes] = gated
        square = square + gated * gated
    mean = jnp.sum(square, axis=1, keepdims=True) * (1.0 / inner)
    scale = lax.rsqrt(mean + norm_epsilon)
    for c in range(blocks):
        lanes = slice(c * LANES, (c + 1) * LANES)
        act[:, lanes] = (diag[:, lanes] * scale * gain[:, lanes]).astype(bf16)
    for start in range(0, width, 256):
        total = None
        for s in range(n_lon):
            term = jnp.dot(
                act[:, s * kr : (s + 1) * kr],
                bo[s, :, start : start + 256],
                preferred_element_type=f32,
            )
            total = term if total is None else total + term
        out[:, start : start + 256] = total.astype(bf16)

    halo.wait_send()
    for i in range(5):
        for k in range(1, n_lon):
            lon_copy(i, k).wait_send()

    def drain(k, carry):
        exchange(k, tbuf, trecv, t_send, t_recv).wait_send()
        exchange(k, sbuf, srecv, s_send, s_recv).wait_send()
        exchange(k, pbuf, precv, p_send, p_recv).wait_send()
        return carry

    lax.fori_loop(1, n_lat, drain, 0)


def local(
    n_lat,
    n_lon,
    fields,
    proj_x,
    proj_z,
    proj_bc,
    proj_dt,
    conv_x,
    conv_bc,
    dt_bias,
    log_rate,
    norm_gain,
    proj_out,
):
    rows, cols, width = fields.shape
    heads = log_rate.shape[0]
    kr, inner = proj_x.shape
    state = proj_bc.shape[1] // 2
    piece = state * inner // LANES // n_lat
    any_spec = pl.BlockSpec(memory_space=pl.ANY)
    vmem = pl.BlockSpec(memory_space=pltpu.VMEM)
    dma = pltpu.SemaphoreType.DMA
    out = pl.pallas_call(
        functools.partial(kernel, n_lat, n_lon, heads),
        out_shape=jax.ShapeDtypeStruct((rows * cols, width), bf16),
        in_specs=[any_spec] * 6 + [vmem] * 5,
        out_specs=vmem,
        scratch_shapes=[
            pltpu.VMEM((HALO + rows, width), bf16),
            pltpu.VMEM((n_lon, kr, inner), bf16),
            pltpu.VMEM((n_lon, kr, inner), bf16),
            pltpu.VMEM((n_lon, kr, 2 * state), bf16),
            pltpu.VMEM((n_lon, kr, heads), bf16),
            pltpu.VMEM((n_lon,) + proj_out.shape, bf16),
            pltpu.VMEM((HALO + rows, inner), f32),
            pltpu.VMEM((rows, inner), f32),
            pltpu.VMEM((HALO + rows, 2 * state), f32),
            pltpu.VMEM((rows, heads), f32),
            pltpu.VMEM((8, LANES), f32),
            pltpu.VMEM((rows, inner), bf16),
            pltpu.VMEM((rows, inner), f32),
            pltpu.VMEM((3, rows, LANES), f32),
            pltpu.VMEM((n_lat, 8, LANES), f32),
            pltpu.VMEM((n_lat, 8, LANES), f32),
            pltpu.VMEM((n_lat, piece, LANES), bf16),
            pltpu.VMEM((n_lat, piece, LANES), bf16),
            pltpu.VMEM((n_lat, piece, LANES), bf16),
            pltpu.VMEM((n_lat, piece, LANES), bf16),
            dma((6,)),
            dma((5, n_lon)),
            dma((5, n_lon)),
            dma,
            dma,
        ]
        + [dma((n_lat,))] * 6,
        compiler_params=pltpu.CompilerParams(
            collective_id=0, has_side_effects=True, vmem_limit_bytes=56 * 1024 * 1024
        ),
    )(
        fields.reshape(rows * cols, width),
        proj_x,
        proj_z,
        proj_bc,
        proj_dt,
        proj_out,
        conv_x,
        conv_bc,
        dt_bias.reshape(1, -1),
        log_rate.reshape(1, -1),
        norm_gain.reshape(1, -1),
    )
    return out.reshape(rows, cols, width)


def solution(mesh):
    rows = P("lon", None)
    return jax.shard_map(
        functools.partial(local, mesh.shape["lat"], mesh.shape["lon"]),
        mesh=mesh,
        in_specs=(P("lat", "lon", None), rows, rows, rows, rows)
        + (P(), P(), P(), P(), P(), rows),
        out_specs=P("lat", "lon", None),
        check_vma=False,
    )
```

```python
import functools

import jax
import jax.numpy as jnp
from jax import lax
from jax.experimental import pallas as pl
from jax.experimental.pallas import tpu as pltpu
from jax.sharding import PartitionSpec as P

norm_epsilon = 1e-05
LANES = 128
HALO = 16
f32 = jnp.float32
bf16 = jnp.bfloat16
highest = lax.Precision.HIGHEST


def silu(v):
    return v / (1.0 + jnp.exp(-v))


def expand(values, spread):
    high = values.astype(bf16)
    low = (values - high.astype(f32)).astype(bf16)
    return jnp.dot(high, spread, preferred_element_type=f32) + jnp.dot(
        low, spread, preferred_element_type=f32
    )


def kernel(
    n_lat,
    n_lon,
    heads,
    fields,
    wx,
    wz,
    wbc,
    wdt,
    wo,
    cx_in,
    cbc_in,
    dtb_in,
    lrate_in,
    gain_in,
    out,
    cx,
    cbc,
    dtb,
    lrate,
    gain,
    fbuf,
    bx,
    bz,
    bbc,
    bdt,
    bo,
    accx,
    accz,
    accbc,
    accdt,
    prm,
    act,
    diag,
    dec,
    tbuf,
    trecv,
    sbuf,
    srecv,
    pbuf,
    precv,
    local_sem,
    lon_send,
    lon_recv,
    halo_send,
    halo_recv,
    t_send,
    t_recv,
    s_send,
    s_recv,
    p_send,
    p_recv,
):
    rows, width = fields.shape
    inner = wx.shape[1]
    state = wbc.shape[1] // 2
    taps = cx_in.shape[0]
    kr = wx.shape[0]
    head_dim = inner // heads
    blocks = inner // LANES
    per_block = LANES // head_dim
    split = n_lat // blocks
    piece = state // split
    me = lax.axis_index("lat")
    col = lax.axis_index("lon")

    barrier = pltpu.get_barrier_semaphore()
    for k in range(1, n_lon):
        pl.semaphore_signal(barrier, inc=1, device_id={"lon": lax.rem(col + k, n_lon)})

    def greet(k, carry):
        pl.semaphore_signal(barrier, inc=1, device_id={"lat": lax.rem(me + k, n_lat)})
        return carry

    lax.fori_loop(1, n_lat, greet, 0)

    weights = ((wbc, bbc), (wdt, bdt), (wx, bx), (wz, bz), (wo, bo))
    own = [pltpu.make_async_copy(fields, fbuf.at[pl.ds(HALO, rows)], local_sem.at[5])]
    for i, (src, dst) in enumerate(weights):
        own.append(pltpu.make_async_copy(src, dst.at[col], local_sem.at[i]))
    small = ((cx_in, cx), (cbc_in, cbc), (dtb_in, dtb), (lrate_in, lrate), (gain_in, gain))
    for i, (src, dst) in enumerate(small):
        own.append(pltpu.make_async_copy(src, dst, local_sem.at[6 + i]))
    for c in own:
        c.start()
    pl.semaphore_wait(barrier, n_lat - 1 + n_lon - 1)

    halo = pltpu.make_async_remote_copy(
        src_ref=fields.at[pl.ds(rows - HALO, HALO)],
        dst_ref=fbuf.at[pl.ds(0, HALO)],
        send_sem=halo_send,
        recv_sem=halo_recv,
        device_id={"lat": lax.rem(me + 1, n_lat)},
    )
    halo.start()

    def lon_copy(i, k):
        src, dst = weights[i]
        return pltpu.make_async_remote_copy(
            src_ref=src,
            dst_ref=dst.at[col],
            send_sem=lon_send.at[i, k],
            recv_sem=lon_recv.at[i, k],
            device_id={"lon": lax.rem(col + k, n_lon)},
        )

    for i in range(5):
        for k in range(1, n_lon):
            lon_copy(i, k).start()

    def part(k):
        source = lax.rem(col + n_lon - k, n_lon)
        return source, pl.ds(pl.multiple_of(source * kr, LANES), kr)

    def arrived(i, k):
        if k > 0:
            lon_copy(i, k).wait_recv()

    for c in own:
        c.wait()
    halo.wait_recv()
    keep = jnp.where(me > 0, 1.0, 0.0).astype(bf16)
    fbuf[0:HALO, :] = fbuf[0:HALO, :] * keep

    def accumulate(k, buf, acc, first_row, step):
        source, columns = part(k)
        lhs = fbuf[first_row:, columns]
        total = buf.shape[2]
        for start in range(0, total, step):
            size = min(step, total - start)
            term = jnp.dot(lhs, buf[source, :, start : start + size], preferred_element_type=f32)
            if k > 0:
                term = term + acc[:, start : start + size]
            if k == n_lon - 1:
                term = term.astype(bf16).astype(f32)
            acc[:, start : start + size] = term

    def accumulate_dt(k):
        source, columns = part(k)
        term = lax.dot_general(
            fbuf[HALO:, columns],
            bdt[source],
            (((1,), (1,)), ((), ())),
            preferred_element_type=f32,
        )
        if k > 0:
            term = term + accdt[...]
        if k == n_lon - 1:
            term = term.astype(bf16).astype(f32)
        accdt[...] = term

    accumulate(0, bbc, accbc, 0, 256)
    accumulate_dt(0)
    accumulate(0, bx, accx, 0, 256)

    for k in range(1, n_lon):
        arrived(0, k)
        accumulate(k, bbc, accbc, 0, 256)
    for k in range(1, n_lon):
        arrived(1, k)
        accumulate_dt(k)

    def conv(acc, kernel_ref, start, size):
        total = None
        for k in range(taps):
            first = HALO - taps + 1 + k
            term = kernel_ref[k : k + 1, start : start + size] * acc[
                first : first + rows, start : start + size
            ]
            total = term if total is None else total + term
        return silu(total)

    bc_act = conv(accbc, cbc, 0, 2 * state)
    lane = lax.broadcasted_iota(jnp.int32, (rows, 2 * state), 1)
    bc16 = bc_act.astype(bf16)
    bc_f = bc16.astype(f32)
    read = pltpu.roll(bc_f, state, 1).astype(bf16)
    b_only = jnp.where(lane < state, bc_f, 0.0).astype(bf16)
    bc_t = bc_f.T.astype(bf16)

    prm[...] = jnp.zeros_like(prm)
    prm[0:1, 0:heads] = dtb[...]
    prm[1:2, 0:heads] = lrate[...]
    dec[0] = jnp.zeros((rows, LANES), f32)
    dec[0, :, 0:heads] = accdt[...]
    pre = dec[0] + prm[0:1, :]
    step_dt = jnp.maximum(pre, 0.0) + jnp.log1p(jnp.exp(-jnp.abs(pre)))
    log_step = -jnp.exp(prm[1:2, :]) * step_dt
    t_idx = lax.broadcasted_iota(jnp.int32, (rows, rows), 0)
    s_idx = lax.broadcasted_iota(jnp.int32, (rows, rows), 1)
    causal = t_idx >= s_idx
    cum = jnp.dot(
        jnp.where(causal, 1.0, 0.0), log_step, precision=highest, preferred_element_type=f32
    )
    dec[0] = cum
    dec[1] = cum.T
    dec[2] = step_dt.T
    band_total = cum[rows - 1 : rows, :]
    spread = jnp.where(
        lax.broadcasted_iota(jnp.int32, (LANES, inner), 1) // head_dim
        == lax.broadcasted_iota(jnp.int32, (LANES, inner), 0),
        1.0,
        0.0,
    ).astype(bf16)
    band_decay = expand(jnp.broadcast_to(jnp.exp(band_total), (8, LANES)), spread)
    for j in range(n_lat):
        c = j % blocks
        tbuf[j] = band_decay[:, c * LANES : (c + 1) * LANES]
    trecv[me] = tbuf[me]

    def exchange(k, buf, dst, send, recv):
        return outgoing(lax.rem(me + k, n_lat), buf, dst, send, recv)

    def outgoing(to, buf, dst, send, recv):
        return pltpu.make_async_remote_copy(
            src_ref=buf.at[to],
            dst_ref=dst.at[me],
            send_sem=send.at[to],
            recv_sem=recv.at[me],
            device_id={"lat": to},
        )

    def incoming(source, buf, dst, send, recv):
        return pltpu.make_async_remote_copy(
            src_ref=buf.at[source],
            dst_ref=dst.at[source],
            send_sem=send.at[source],
            recv_sem=recv.at[source],
            device_id={"lat": source},
        )

    def send_t(k, carry):
        exchange(k, tbuf, trecv, t_send, t_recv).start()
        return carry

    lax.fori_loop(1, n_lat, send_t, 0)

    scores = lax.dot_general(
        read, b_only, (((1,), (1,)), ((), ())), preferred_element_type=f32
    )
    end_weight = expand(jnp.exp(band_total - cum) * step_dt, spread)

    for k in range(1, n_lon):
        arrived(2, k)
        accumulate(k, bx, accx, 0, 256)
    for c in range(blocks):
        lanes = slice(c * LANES, (c + 1) * LANES)
        block = conv(accx, cx, c * LANES, LANES).astype(bf16)
        act[:, lanes] = block
        weighted = (block.astype(f32) * end_weight[:, lanes]).astype(bf16)
        end_state = jnp.dot(bc_t, weighted, preferred_element_type=f32)
        for r in range(split):
            to = r * blocks + c
            sbuf[to] = end_state[r * piece : (r + 1) * piece, :].astype(bf16)

            @pl.when(me != to)
            def _():
                outgoing(to, sbuf, srecv, s_send, s_recv).start()

    srecv[me] = sbuf[me]

    half = lax.broadcasted_iota(jnp.int32, (rows, LANES), 1) // head_dim
    for c in range(blocks):
        lanes = slice(c * LANES, (c + 1) * LANES)
        mixed = None
        for g in range(per_block):
            h = c * per_block + g
            gap = dec[0, :, h : h + 1] - dec[1, h : h + 1, :]
            decay = jnp.exp(jnp.where(causal, gap, -jnp.inf))
            mix = (decay * scores * dec[2, h : h + 1, :]).astype(bf16)
            term = jnp.dot(mix, act[:, lanes], preferred_element_type=f32)
            mixed = term if mixed is None else jnp.where(half == g, term, mixed)
        diag[:, lanes] = mixed
    start_decay = jnp.exp(cum)

    carried = jnp.zeros((piece, LANES), f32)
    for d in range(n_lat):

        @pl.when(me != d)
        def _():
            incoming(d, tbuf, trecv, t_send, t_recv).wait_recv()
            incoming(d, sbuf, srecv, s_send, s_recv).wait_recv()

        pbuf[d] = carried.astype(bf16)

        @pl.when(me != d)
        def _():
            outgoing(d, pbuf, precv, p_send, p_recv).start()

        carried = trecv[d][0:1, :] * carried + srecv[d].astype(f32)
    precv[me] = pbuf[me]

    accumulate(0, bz, accz, HALO, 256)
    for k in range(1, n_lon):
        arrived(3, k)
        accumulate(k, bz, accz, HALO, 256)
    for c in range(blocks):
        lanes = slice(c * LANES, (c + 1) * LANES)
        accz[:, lanes] = silu(accz[:, lanes])
        accx[0:rows, lanes] = expand(start_decay, spread[:, lanes])
    for k in range(1, n_lon):
        arrived(4, k)

    def take_p(k, carry):
        incoming(lax.rem(me + k, n_lat), pbuf, precv, p_send, p_recv).wait_recv()
        return carry

    lax.fori_loop(1, n_lat, take_p, 0)

    square = jnp.zeros((rows, LANES), f32)
    for c in range(blocks):
        lanes = slice(c * LANES, (c + 1) * LANES)
        prefix = jnp.concatenate([precv[r * blocks + c] for r in range(split)], axis=0)
        lower = jnp.concatenate([jnp.zeros_like(prefix), prefix], axis=0)
        y = jnp.dot(bc16, lower, preferred_element_type=f32) * accx[0:rows, lanes] + diag[:, lanes]
        gated = y * accz[:, lanes]
        diag[:, lanes] = gated
        square = square + gated * gated
    mean = jnp.sum(square, axis=1, keepdims=True) * (1.0 / inner)
    scale = lax.rsqrt(mean + norm_epsilon)
    for c in range(blocks):
        lanes = slice(c * LANES, (c + 1) * LANES)
        act[:, lanes] = (diag[:, lanes] * scale * gain[:, lanes]).astype(bf16)
    for start in range(0, width, 256):
        total = None
        for s in range(n_lon):
            term = jnp.dot(
                act[:, s * kr : (s + 1) * kr],
                bo[s, :, start : start + 256],
                preferred_element_type=f32,
            )
            total = term if total is None else total + term
        out[:, start : start + 256] = total.astype(bf16)

    halo.wait_send()
    for i in range(5):
        for k in range(1, n_lon):
            lon_copy(i, k).wait_send()

    def drain(k, carry):
        exchange(k, tbuf, trecv, t_send, t_recv).wait_send()
        exchange(k, sbuf, srecv, s_send, s_recv).wait_send()
        exchange(k, pbuf, precv, p_send, p_recv).wait_send()
        return carry

    lax.fori_loop(1, n_lat, drain, 0)


def local(
    n_lat,
    n_lon,
    fields,
    proj_x,
    proj_z,
    proj_bc,
    proj_dt,
    conv_x,
    conv_bc,
    dt_bias,
    log_rate,
    norm_gain,
    proj_out,
):
    rows, cols, width = fields.shape
    heads = log_rate.shape[0]
    kr, inner = proj_x.shape
    state = proj_bc.shape[1] // 2
    piece = state * inner // LANES // n_lat
    operands = (
        fields.reshape(rows * cols, width),
        proj_x,
        proj_z,
        proj_bc,
        proj_dt.T,
        proj_out,
        conv_x,
        conv_bc,
        dt_bias.reshape(1, -1),
        log_rate.reshape(1, -1),
        norm_gain.reshape(1, -1),
    )
    hbm = pl.BlockSpec(memory_space=pl.ANY)
    vmem = pl.BlockSpec(memory_space=pltpu.VMEM)
    dma = pltpu.SemaphoreType.DMA
    out = pl.pallas_call(
        functools.partial(kernel, n_lat, n_lon, heads),
        out_shape=jax.ShapeDtypeStruct((rows * cols, width), bf16),
        in_specs=[hbm] * 11,
        out_specs=vmem,
        scratch_shapes=[
            pltpu.VMEM(conv_x.shape, f32),
            pltpu.VMEM(conv_bc.shape, f32),
            pltpu.VMEM((1, heads), f32),
            pltpu.VMEM((1, heads), f32),
            pltpu.VMEM((1, inner), f32),
            pltpu.VMEM((HALO + rows, width), bf16),
            pltpu.VMEM((n_lon, kr, inner), bf16),
            pltpu.VMEM((n_lon, kr, inner), bf16),
            pltpu.VMEM((n_lon, kr, 2 * state), bf16),
            pltpu.VMEM((n_lon, heads, kr), bf16),
            pltpu.VMEM((n_lon,) + proj_out.shape, bf16),
            pltpu.VMEM((HALO + rows, inner), f32),
            pltpu.VMEM((rows, inner), f32),
            pltpu.VMEM((HALO + rows, 2 * state), f32),
            pltpu.VMEM((rows, heads), f32),
            pltpu.VMEM((8, LANES), f32),
            pltpu.VMEM((rows, inner), bf16),
            pltpu.VMEM((rows, inner), f32),
            pltpu.VMEM((3, rows, LANES), f32),
            pltpu.VMEM((n_lat, 8, LANES), f32),
            pltpu.VMEM((n_lat, 8, LANES), f32),
            pltpu.VMEM((n_lat, piece, LANES), bf16),
            pltpu.VMEM((n_lat, piece, LANES), bf16),
            pltpu.VMEM((n_lat, piece, LANES), bf16),
            pltpu.VMEM((n_lat, piece, LANES), bf16),
            dma((11,)),
            dma((5, n_lon)),
            dma((5, n_lon)),
            dma,
            dma,
        ]
        + [dma((n_lat,))] * 6,
        compiler_params=pltpu.CompilerParams(
            collective_id=0, has_side_effects=True, vmem_limit_bytes=16 * 1024 * 1024
        ),
    )(
        *(pltpu.with_memory_space_constraint(v, pltpu.HBM) for v in operands)
    )
    return out.reshape(rows, cols, width)


def solution(mesh):
    rows = P("lon", None)
    return jax.shard_map(
        functools.partial(local, mesh.shape["lat"], mesh.shape["lon"]),
        mesh=mesh,
        in_specs=(P("lat", "lon", None), rows, rows, rows, rows)
        + (P(), P(), P(), P(), P(), rows),
        out_specs=P("lat", "lon", None),
        check_vma=False,
    )
```

```python
import functools

import jax
import jax.numpy as jnp
from jax import lax
from jax.experimental import pallas as pl
from jax.experimental.pallas import tpu as pltpu
from jax.sharding import PartitionSpec as P

norm_epsilon = 1e-05
LANES = 128
HALO = 16
f32 = jnp.float32
bf16 = jnp.bfloat16
highest = lax.Precision.HIGHEST


def silu(v):
    return v / (1.0 + jnp.exp(-v))


def expand(values, spread):
    high = values.astype(bf16)
    low = (values - high.astype(f32)).astype(bf16)
    return jnp.dot(high, spread, preferred_element_type=f32) + jnp.dot(
        low, spread, preferred_element_type=f32
    )


def kernel(
    n_lat,
    n_lon,
    heads,
    fields,
    wx,
    wz,
    wbc,
    wdt,
    wo,
    cx_in,
    cbc_in,
    dtb_in,
    lrate_in,
    gain_in,
    out,
    cx,
    cbc,
    dtb,
    lrate,
    gain,
    fbuf,
    bx,
    bz,
    bbc,
    bdt,
    bo,
    accx,
    accz,
    accbc,
    accdt,
    prm,
    act,
    diag,
    dec,
    tbuf,
    trecv,
    sbuf,
    srecv,
    pbuf,
    precv,
    local_sem,
    lon_send,
    lon_recv,
    halo_send,
    halo_recv,
    t_send,
    t_recv,
    s_send,
    s_recv,
    p_send,
    p_recv,
):
    rows, width = fields.shape
    inner = wx.shape[1]
    state = wbc.shape[1] // 2
    taps = cx_in.shape[0]
    kr = wx.shape[0]
    head_dim = inner // heads
    blocks = inner // LANES
    per_block = LANES // head_dim
    split = n_lat // blocks
    piece = state // split
    me = lax.axis_index("lat")
    col = lax.axis_index("lon")

    barrier = pltpu.get_barrier_semaphore()
    for k in range(1, n_lon):
        pl.semaphore_signal(barrier, inc=1, device_id={"lon": lax.rem(col + k, n_lon)})

    def greet(k, carry):
        pl.semaphore_signal(barrier, inc=1, device_id={"lat": lax.rem(me + k, n_lat)})
        return carry

    lax.fori_loop(1, n_lat, greet, 0)

    weights = ((wbc, bbc), (wdt, bdt), (wx, bx), (wz, bz), (wo, bo))
    own = [pltpu.make_async_copy(fields, fbuf.at[pl.ds(HALO, rows)], local_sem.at[5])]
    for i, (src, dst) in enumerate(weights):
        own.append(pltpu.make_async_copy(src, dst.at[col], local_sem.at[i]))
    small = ((cx_in, cx), (cbc_in, cbc), (dtb_in, dtb), (lrate_in, lrate), (gain_in, gain))
    for i, (src, dst) in enumerate(small):
        own.append(pltpu.make_async_copy(src, dst, local_sem.at[6 + i]))
    for c in own:
        c.start()
    pl.semaphore_wait(barrier, n_lat - 1 + n_lon - 1)

    halo = pltpu.make_async_remote_copy(
        src_ref=fields.at[pl.ds(rows - HALO, HALO)],
        dst_ref=fbuf.at[pl.ds(0, HALO)],
        send_sem=halo_send,
        recv_sem=halo_recv,
        device_id={"lat": lax.rem(me + 1, n_lat)},
    )
    halo.start()

    def lon_copy(i, k):
        src, dst = weights[i]
        return pltpu.make_async_remote_copy(
            src_ref=src,
            dst_ref=dst.at[col],
            send_sem=lon_send.at[i, k],
            recv_sem=lon_recv.at[i, k],
            device_id={"lon": lax.rem(col + k, n_lon)},
        )

    for i in range(5):
        for k in range(1, n_lon):
            lon_copy(i, k).start()

    def part(k):
        source = lax.rem(col + n_lon - k, n_lon)
        return source, pl.ds(pl.multiple_of(source * kr, LANES), kr)

    def arrived(i, k):
        if k > 0:
            lon_copy(i, k).wait_recv()

    for c in own:
        c.wait()
    halo.wait_recv()
    keep = jnp.where(me > 0, 1.0, 0.0).astype(bf16)
    fbuf[0:HALO, :] = fbuf[0:HALO, :] * keep

    def accumulate(k, buf, acc, first_row, step):
        source, columns = part(k)
        lhs = fbuf[first_row:, columns]
        total = buf.shape[2]
        for start in range(0, total, step):
            size = min(step, total - start)
            term = jnp.dot(lhs, buf[source, :, start : start + size], preferred_element_type=f32)
            if k > 0:
                term = term + acc[:, start : start + size]
            if k == n_lon - 1:
                term = term.astype(bf16).astype(f32)
            acc[:, start : start + size] = term

    def accumulate_dt(k):
        source, columns = part(k)
        term = lax.dot_general(
            fbuf[HALO:, columns],
            bdt[source],
            (((1,), (1,)), ((), ())),
            preferred_element_type=f32,
        )
        if k > 0:
            term = term + accdt[...]
        if k == n_lon - 1:
            term = term.astype(bf16).astype(f32)
        accdt[...] = term

    accumulate(0, bbc, accbc, 0, 256)
    accumulate_dt(0)
    accumulate(0, bx, accx, 0, 256)

    for k in range(1, n_lon):
        arrived(0, k)
        accumulate(k, bbc, accbc, 0, 256)
    for k in range(1, n_lon):
        arrived(1, k)
        accumulate_dt(k)

    def conv(acc, kernel_ref, start, size):
        total = None
        for k in range(taps):
            first = HALO - taps + 1 + k
            term = kernel_ref[k : k + 1, start : start + size] * acc[
                first : first + rows, start : start + size
            ]
            total = term if total is None else total + term
        return silu(total)

    bc_act = conv(accbc, cbc, 0, 2 * state)
    lane = lax.broadcasted_iota(jnp.int32, (rows, 2 * state), 1)
    bc16 = bc_act.astype(bf16)
    bc_f = bc16.astype(f32)
    bc_t = bc_f.T.astype(bf16)

    prm[...] = jnp.zeros_like(prm)
    prm[0:1, 0:heads] = dtb[...]
    prm[1:2, 0:heads] = lrate[...]
    dec[0] = jnp.zeros((rows, LANES), f32)
    dec[0, :, 0:heads] = accdt[...]
    pre = dec[0] + prm[0:1, :]
    step_dt = jnp.maximum(pre, 0.0) + jnp.log1p(jnp.exp(-jnp.abs(pre)))
    log_step = -jnp.exp(prm[1:2, :]) * step_dt
    t_idx = lax.broadcasted_iota(jnp.int32, (rows, rows), 0)
    s_idx = lax.broadcasted_iota(jnp.int32, (rows, rows), 1)
    causal = t_idx >= s_idx
    cum = jnp.dot(
        jnp.where(causal, 1.0, 0.0), log_step, precision=highest, preferred_element_type=f32
    )
    dec[0] = cum
    dec[1] = step_dt
    band_total = cum[rows - 1 : rows, :]
    spread = jnp.where(
        lax.broadcasted_iota(jnp.int32, (LANES, inner), 1) // head_dim
        == lax.broadcasted_iota(jnp.int32, (LANES, inner), 0),
        1.0,
        0.0,
    ).astype(bf16)
    band_decay = expand(jnp.broadcast_to(jnp.exp(band_total), (8, LANES)), spread)
    for j in range(n_lat):
        c = j % blocks
        tbuf[j] = band_decay[:, c * LANES : (c + 1) * LANES]
    trecv[me] = tbuf[me]

    def exchange(k, buf, dst, send, recv):
        return outgoing(lax.rem(me + k, n_lat), buf, dst, send, recv)

    def outgoing(to, buf, dst, send, recv):
        return pltpu.make_async_remote_copy(
            src_ref=buf.at[to],
            dst_ref=dst.at[me],
            send_sem=send.at[to],
            recv_sem=recv.at[me],
            device_id={"lat": to},
        )

    def incoming(source, buf, dst, send, recv):
        return pltpu.make_async_remote_copy(
            src_ref=buf.at[source],
            dst_ref=dst.at[source],
            send_sem=send.at[source],
            recv_sem=recv.at[source],
            device_id={"lat": source},
        )

    def send_t(k, carry):
        exchange(k, tbuf, trecv, t_send, t_recv).start()
        return carry

    lax.fori_loop(1, n_lat, send_t, 0)

    end_weight = expand(jnp.exp(band_total - cum) * step_dt, spread)

    for k in range(1, n_lon):
        arrived(2, k)
        accumulate(k, bx, accx, 0, 256)
    for c in range(blocks):
        lanes = slice(c * LANES, (c + 1) * LANES)
        block = conv(accx, cx, c * LANES, LANES).astype(bf16)
        act[:, lanes] = block
        weighted = (block.astype(f32) * end_weight[:, lanes]).astype(bf16)
        end_state = jnp.dot(bc_t, weighted, preferred_element_type=f32)
        for r in range(split):
            to = r * blocks + c
            sbuf[to] = end_state[r * piece : (r + 1) * piece, :].astype(bf16)

            @pl.when(me != to)
            def _():
                outgoing(to, sbuf, srecv, s_send, s_recv).start()

    srecv[me] = sbuf[me]

    read = pltpu.roll(bc_f, state, 1).astype(bf16)
    b_only = jnp.where(lane < state, bc_f, 0.0).astype(bf16)
    scores = lax.dot_general(
        read, b_only, (((1,), (1,)), ((), ())), preferred_element_type=f32
    )
    dec[2] = dec[1].T
    dec[1] = dec[0].T
    half = lax.broadcasted_iota(jnp.int32, (rows, LANES), 1) // head_dim
    for c in range(blocks):
        lanes = slice(c * LANES, (c + 1) * LANES)
        mixed = None
        for g in range(per_block):
            h = c * per_block + g
            gap = dec[0, :, h : h + 1] - dec[1, h : h + 1, :]
            decay = jnp.exp(jnp.where(causal, gap, -jnp.inf))
            mix = (decay * scores * dec[2, h : h + 1, :]).astype(bf16)
            term = jnp.dot(mix, act[:, lanes], preferred_element_type=f32)
            mixed = term if mixed is None else jnp.where(half == g, term, mixed)
        diag[:, lanes] = mixed
    start_decay = jnp.exp(dec[0])

    carried = jnp.zeros((piece, LANES), f32)
    for d in range(n_lat):

        @pl.when(me != d)
        def _():
            incoming(d, tbuf, trecv, t_send, t_recv).wait_recv()
            incoming(d, sbuf, srecv, s_send, s_recv).wait_recv()

        pbuf[d] = carried.astype(bf16)

        @pl.when(me != d)
        def _():
            outgoing(d, pbuf, precv, p_send, p_recv).start()

        carried = trecv[d][0:1, :] * carried + srecv[d].astype(f32)
    precv[me] = pbuf[me]

    accumulate(0, bz, accz, HALO, 256)
    for k in range(1, n_lon):
        arrived(3, k)
        accumulate(k, bz, accz, HALO, 256)
    for c in range(blocks):
        lanes = slice(c * LANES, (c + 1) * LANES)
        accz[:, lanes] = silu(accz[:, lanes])
        accx[0:rows, lanes] = expand(start_decay, spread[:, lanes])
    for k in range(1, n_lon):
        arrived(4, k)

    def take_p(k, carry):
        incoming(lax.rem(me + k, n_lat), pbuf, precv, p_send, p_recv).wait_recv()
        return carry

    lax.fori_loop(1, n_lat, take_p, 0)

    square = jnp.zeros((rows, LANES), f32)
    for c in range(blocks):
        lanes = slice(c * LANES, (c + 1) * LANES)
        prefix = jnp.concatenate([precv[r * blocks + c] for r in range(split)], axis=0)
        lower = jnp.concatenate([jnp.zeros_like(prefix), prefix], axis=0)
        y = jnp.dot(bc16, lower, preferred_element_type=f32) * accx[0:rows, lanes] + diag[:, lanes]
        gated = y * accz[:, lanes]
        act[:, lanes] = (gated * gain[:, lanes]).astype(bf16)
        square = square + gated * gated
    mean = jnp.sum(square, axis=1, keepdims=True) * (1.0 / inner)
    scale = lax.rsqrt(mean + norm_epsilon)
    for start in range(0, width, 256):
        total = None
        for s in range(n_lon):
            term = jnp.dot(
                act[:, s * kr : (s + 1) * kr],
                bo[s, :, start : start + 256],
                preferred_element_type=f32,
            )
            total = term if total is None else total + term
        out[:, start : start + 256] = (total * scale).astype(bf16)

    halo.wait_send()
    for i in range(5):
        for k in range(1, n_lon):
            lon_copy(i, k).wait_send()

    def drain(k, carry):
        exchange(k, tbuf, trecv, t_send, t_recv).wait_send()
        exchange(k, sbuf, srecv, s_send, s_recv).wait_send()
        exchange(k, pbuf, precv, p_send, p_recv).wait_send()
        return carry

    lax.fori_loop(1, n_lat, drain, 0)


def local(
    n_lat,
    n_lon,
    fields,
    proj_x,
    proj_z,
    proj_bc,
    proj_dt,
    conv_x,
    conv_bc,
    dt_bias,
    log_rate,
    norm_gain,
    proj_out,
):
    rows, cols, width = fields.shape
    heads = log_rate.shape[0]
    kr, inner = proj_x.shape
    state = proj_bc.shape[1] // 2
    piece = state * inner // LANES // n_lat
    operands = (
        fields.reshape(rows * cols, width),
        proj_x,
        proj_z,
        proj_bc,
        proj_dt.T,
        proj_out,
        conv_x,
        conv_bc,
        dt_bias.reshape(1, -1),
        log_rate.reshape(1, -1),
        norm_gain.reshape(1, -1),
    )
    hbm = pl.BlockSpec(memory_space=pl.ANY)
    vmem = pl.BlockSpec(memory_space=pltpu.VMEM)
    dma = pltpu.SemaphoreType.DMA
    out = pl.pallas_call(
        functools.partial(kernel, n_lat, n_lon, heads),
        out_shape=jax.ShapeDtypeStruct((rows * cols, width), bf16),
        in_specs=[hbm] * 11,
        out_specs=vmem,
        scratch_shapes=[
            pltpu.VMEM(conv_x.shape, f32),
            pltpu.VMEM(conv_bc.shape, f32),
            pltpu.VMEM((1, heads), f32),
            pltpu.VMEM((1, heads), f32),
            pltpu.VMEM((1, inner), f32),
            pltpu.VMEM((HALO + rows, width), bf16),
            pltpu.VMEM((n_lon, kr, inner), bf16),
            pltpu.VMEM((n_lon, kr, inner), bf16),
            pltpu.VMEM((n_lon, kr, 2 * state), bf16),
            pltpu.VMEM((n_lon, heads, kr), bf16),
            pltpu.VMEM((n_lon,) + proj_out.shape, bf16),
            pltpu.VMEM((HALO + rows, inner), f32),
            pltpu.VMEM((rows, inner), f32),
            pltpu.VMEM((HALO + rows, 2 * state), f32),
            pltpu.VMEM((rows, heads), f32),
            pltpu.VMEM((8, LANES), f32),
            pltpu.VMEM((rows, inner), bf16),
            pltpu.VMEM((rows, inner), f32),
            pltpu.VMEM((3, rows, LANES), f32),
            pltpu.VMEM((n_lat, 8, LANES), f32),
            pltpu.VMEM((n_lat, 8, LANES), f32),
            pltpu.VMEM((n_lat, piece, LANES), bf16),
            pltpu.VMEM((n_lat, piece, LANES), bf16),
            pltpu.VMEM((n_lat, piece, LANES), bf16),
            pltpu.VMEM((n_lat, piece, LANES), bf16),
            dma((11,)),
            dma((5, n_lon)),
            dma((5, n_lon)),
            dma,
            dma,
        ]
        + [dma((n_lat,))] * 6,
        compiler_params=pltpu.CompilerParams(
            collective_id=0, has_side_effects=True, vmem_limit_bytes=16 * 1024 * 1024
        ),
    )(
        *(pltpu.with_memory_space_constraint(v, pltpu.HBM) for v in operands)
    )
    return out.reshape(rows, cols, width)


def solution(mesh):
    rows = P("lon", None)
    return jax.shard_map(
        functools.partial(local, mesh.shape["lat"], mesh.shape["lon"]),
        mesh=mesh,
        in_specs=(P("lat", "lon", None), rows, rows, rows, rows)
        + (P(), P(), P(), P(), P(), rows),
        out_specs=P("lat", "lon", None),
        check_vma=False,
    )
```
